32 devices in a mesh: orient: 8 (over z, y), dom: 4 (over x, core).
Axes of the slice: x: 2, y: 2, z: 4, core: 2. Of those that a mesh axis runs over, the one named last changes fastest.
Arguments:
- particles: bfloat16 [256, 8448], P(('dom', 'orient')), parts along dimension 0, may hold values from -12 to 12
- defocus: float32 [256], P(('dom', 'orient')), parts along dimension 0, may hold values from 10 to 60
- inv_noise: float32 [4224], replicated, may hold values from 0.5 to 2
- references: bfloat16 [13824, 8448], P(('dom', 'orient')), parts along dimension 0, may hold values from -0.25 to 0.25
- thresholds: int32 [256], P('dom'), parts along dimension 0, may hold values from 512 to 1023
- range_start: int32 [256], P('dom'), parts along dimension 0, may hold values from 0 to 3455
- range_len: int32 [256], P('dom'), parts along dimension 0, may hold values from 36 to 1727
Outputs:
- posterior: float32 [256, 3456], P('dom', 'orient'), parts along dimension 0
- cumulative: float32 [256, 3456], P('dom', 'orient'), parts along dimension 0
- log_evidence: float32 [256], P('dom'), parts along dimension 0
- kept_mass: float32 [256], P('dom'), parts along dimension 0
The draws below stay inside these ranges and needn't reach their ends.
There are 4 independent parts, one for each index of `dom`. The reference program is written for one: setup_inputs(seed, part) draws one part's arguments, and reference() takes and returns one part's arrays. A program takes and returns all parts, laid end to end along the dimension named above; an argument that names none is the same for every part. Nothing has to cross between parts.
All inputs are finite; a program needn't handle non-finite values.
Results may differ from the reference program's by a relative error of at most 0.0004.
The reference program's roundings to bfloat16 on the way (of `weighted`, `ctf_power` and `power`) count: a program that leaves them out, or rounds other values in their place, can miss the bound.
Values may be sent and summed in bfloat16 or wider, within the bound.
A program may use at most 64 MiB of HBM per device.

```python
import math
import jax
import jax.numpy as jnp
from jax import lax

COEF = 4224
FEAT = 8448
ROT = 36
ORIENTS = 3456
P_SIZE = 64


def ctf_rows(defocus, coef):
    index = jnp.arange(coef, dtype=jnp.int32)
    row_pos = (index // 128).astype(jnp.float32)
    col_pos = (index % 128 - 64).astype(jnp.float32)
    freq = math.pi * (row_pos * row_pos + col_pos * col_pos) / 16384.0
    return -jnp.sin(defocus[:, None] * freq[None, :] + 0.07)


def strong_rows(key):
    return jax.random.randint(jax.random.fold_in(key, 15), (8,), 0, ORIENTS)


def ref_row(key, row, strong):
    row_key = jax.random.fold_in(jax.random.fold_in(key, 11), row)
    spread = jnp.exp(jax.random.uniform(jax.random.fold_in(row_key, 1), (), jnp.float32, math.log(0.7), math.log(1.4)))
    base = jax.random.normal(jax.random.fold_in(row_key, 2), (FEAT,), jnp.float32)
    is_strong = jnp.any(strong == row)
    amplitude = jnp.where(is_strong, 0.12, 0.02)
    return jnp.clip(amplitude * spread * base, -0.25, 0.25)


def defocus_of(key):
    return jax.random.uniform(jax.random.fold_in(key, 12), (P_SIZE,), jnp.float32, 20.0, 50.0)


def draw_references(key, part):
    strong = strong_rows(key)
    rows_all = jnp.arange(ORIENTS, dtype=jnp.int32)
    return jax.vmap(lambda row: ref_row(key, row, strong))(rows_all).astype(jnp.bfloat16)


def draw_defocus(key, part):
    return defocus_of(key)


def draw_particles(key, part):
    images = jax.random.normal(jax.random.fold_in(key, 13), (P_SIZE, FEAT), jnp.float32)
    strong = strong_rows(key)
    chosen = jax.random.randint(jax.random.fold_in(key, 14), (4,), 0, P_SIZE)
    targets = jax.random.uniform(jax.random.fold_in(key, 16), (4,), jnp.float32, 110.0, 250.0)
    first_rows = jax.vmap(lambda row: ref_row(key, row, strong))(strong[:4])
    second_rows = jax.vmap(lambda row: ref_row(key, row, strong))(strong[4:])
    ctf = ctf_rows(defocus_of(key)[chosen], FEAT // 2)
    ctf_both = jnp.concatenate([ctf, ctf], axis=1)
    gain_first = targets / (0.0078 * FEAT)
    gain_second = (targets - 2.0) / (0.0078 * FEAT)
    aligned = 0.3 * images[chosen] + ctf_both * (gain_first[:, None] * first_rows + gain_second[:, None] * second_rows)
    images = images.at[chosen].set(aligned)
    return jnp.clip(images, -12.0, 12.0).astype(jnp.bfloat16)


def place_ends(result, stream_key, low, largest):
    shape = result.shape
    spot = [jax.random.randint(jax.random.fold_in(stream_key, axis), (), 0, shape[axis]) for axis in range(len(shape))]
    result = result.at[tuple(spot)].set(low)
    longest = shape.index(max(shape))
    spot[longest] = (spot[longest] + 1) % shape[longest]
    return result.at[tuple(spot)].set(largest)


def setup_inputs(seed: int = 0, part: int = 0) -> dict:
    key_of = jax.random.split(jax.random.key(seed), 8)
    part_keys = jax.random.split(jax.random.fold_in(key_of[7], part), 8)
    particles = draw_particles(jax.random.fold_in(jax.random.fold_in(key_of[7], part), 71), part)
    defocus = draw_defocus(jax.random.fold_in(jax.random.fold_in(key_of[7], part), 71), part)
    inv_noise = jnp.clip(jnp.exp(jax.random.uniform(key_of[2], (COEF,), jnp.float32, math.log(0.5), math.log(2.0))), 0.5, 2.0)
    references = draw_references(jax.random.fold_in(jax.random.fold_in(key_of[7], part), 71), part)
    thresholds = place_ends(jax.random.randint(part_keys[4], (P_SIZE,), 512, 1024), jax.random.fold_in(part_keys[4], 1), 512, 1023).astype(jnp.int32)
    range_start = place_ends(jax.random.randint(part_keys[5], (P_SIZE,), 0, ORIENTS), jax.random.fold_in(part_keys[5], 1), 0, ORIENTS - 1).astype(jnp.int32)
    range_len = place_ends(jax.random.randint(part_keys[6], (P_SIZE,), ROT, ORIENTS // 2), jax.random.fold_in(part_keys[6], 1), ROT, (ORIENTS // 2) - 1).astype(jnp.int32)
    return dict(particles=particles, defocus=defocus, inv_noise=inv_noise, references=references, thresholds=thresholds, range_start=range_start, range_len=range_len)


def ctf_table(defocus, coef):
    index = jnp.arange(coef, dtype=jnp.int32)
    row_pos = (index // 128).astype(jnp.float32)
    col_pos = (index % 128 - 64).astype(jnp.float32)
    freq = math.pi * (row_pos * row_pos + col_pos * col_pos) / 16384.0
    return -jnp.sin(defocus[:, None] * freq[None, :] + 0.07)


def reference(particles, defocus, inv_noise, references, thresholds, range_start, range_len):
    coef = inv_noise.shape[0]
    ctf = ctf_table(defocus, coef)
    ctf_both = jnp.concatenate([ctf, ctf], axis=1)
    noise_both = jnp.concatenate([inv_noise, inv_noise])
    weighted = (particles.astype(jnp.float32) * ctf_both * noise_both[None, :]).astype(jnp.bfloat16)
    ctf_power = (ctf * ctf * inv_noise[None, :]).astype(jnp.bfloat16)
    real_part = references[:, :coef].astype(jnp.float32)
    imag_part = references[:, coef:].astype(jnp.float32)
    power = (real_part * real_part + imag_part * imag_part).astype(jnp.bfloat16)
    dims = (((1,), (1,)), ((), ()))
    scores = lax.dot_general(weighted, references, dims, preferred_element_type=jnp.float32)
    scores = scores - 0.5 * lax.dot_general(ctf_power, power, dims, preferred_element_type=jnp.float32)
    top_score = jnp.max(scores, axis=1)
    expon = jnp.exp(scores - top_score[:, None])
    total = jnp.sum(expon, axis=1)
    posterior = expon / total[:, None]
    cumulative = jnp.cumsum(posterior, axis=1)
    before = cumulative - posterior
    fraction = thresholds.astype(jnp.float32) / 1024.0
    kept = jnp.minimum(jnp.maximum(fraction[:, None] - before, 0.0), posterior)
    orient_ids = jnp.arange(ORIENTS, dtype=jnp.int32)
    inside = ((orient_ids[None, :] - range_start[:, None]) % ORIENTS) < range_len[:, None]
    kept_mass = jnp.sum(jnp.where(inside, kept, 0.0), axis=1)
    log_evidence = top_score + jnp.log(total)
    return posterior, cumulative, log_evidence, kept_mass
```

```python
import functools
import math

import jax
import jax.numpy as jnp
from jax import lax
from jax.experimental import pallas as pl
from jax.experimental.pallas import tpu as pltpu
from jax.sharding import PartitionSpec as P

MESH = pl.DeviceIdType.MESH
DIMS = (((1,), (1,)), ((), ()))
PIECES = 3
ROWS = 16


def sin_of(x):
    k = jnp.floor(x * (1.0 / math.pi) + 0.5)
    r = x - k * 3.140625
    r = r - k * 9.67502593994140625e-4
    r = r - k * 1.509957990978376432e-7
    s = r * r
    p = jnp.float32(-2.3889859e-8)
    p = p * s + 2.7525562e-6
    p = p * s - 1.9840874e-4
    p = p * s + 8.3333310e-3
    p = p * s - 1.6666667e-1
    y = r + r * s * p
    half = k * 0.5
    return jnp.where(half == jnp.floor(half), y, -y)


def loop(count, body):
    if count <= 4:
        for i in range(count):
            body(i)
    else:
        def step(i, carry):
            body(i)
            return carry
        lax.fori_loop(0, count, step, 0)


def kernel(
    n, particles, defocus, noise, references, thresholds, starts, lens,
    posterior, cumulative, evidence, kept_mass,
    gath, dgath, refs, ctf, ctf_power, power, weighted, acc, expon, prefix, mine, sgath,
    own_sem, ref_sem, z_send, z_recv, y_send, y_recv, d_send, d_recv, s_send, s_recv,
):
    wide = 2 if n % 2 == 0 else 1
    deep = n // wide
    per = particles.shape[0]
    feat = particles.shape[1]
    coef = feat // 2
    size = coef // PIECES
    chunks = 2 * PIECES
    ori = references.shape[0]
    total_ori = n * ori
    parts = n * per
    me = lax.axis_index("orient")
    row = lax.div(me, wide)
    col = lax.rem(me, wide)

    def cut(c):
        return pl.ds(c * size, size)

    def peer(t):
        return lax.rem(me + t, n)

    barrier = pltpu.get_barrier_semaphore()
    for t in range(1, n):
        pl.semaphore_signal(barrier, inc=1, device_id={"orient": peer(t)}, device_id_type=MESH)

    own = pltpu.make_async_copy(particles, gath.at[me], own_sem.at[0])
    own.start()
    own_d = pltpu.make_async_copy(defocus, dgath.at[me], own_sem.at[1])
    own_d.start()
    order = [c for k in range(PIECES) for c in (k, k + PIECES)]
    loads = {}
    for c in order:
        loads[c] = pltpu.make_async_copy(references.at[:, cut(c)], refs.at[:, cut(c)], ref_sem.at[c])
        loads[c].start()
    own.wait()
    own_d.wait()
    pl.semaphore_wait(barrier, n - 1)

    def d_copy(source, target):
        return pltpu.make_async_remote_copy(
            src_ref=dgath.at[source], dst_ref=dgath.at[source],
            send_sem=d_send.at[target], recv_sem=d_recv.at[source],
            device_id={"orient": target}, device_id_type=MESH)

    def z_copy(c, source_row, target_row):
        block = gath.at[source_row * wide + col, :, cut(c)]
        return pltpu.make_async_remote_copy(
            src_ref=block, dst_ref=block,
            send_sem=z_send.at[c, target_row], recv_sem=z_recv.at[c, source_row],
            device_id={"orient": target_row * wide + col}, device_id_type=MESH)

    def y_copy(c, source_row, source_col):
        block = gath.at[source_row * wide + source_col, :, cut(c)]
        return pltpu.make_async_remote_copy(
            src_ref=block, dst_ref=block,
            send_sem=y_send.at[c, source_row], recv_sem=y_recv.at[c, source_row],
            device_id={"orient": row * wide + (wide - 1 - col)}, device_id_type=MESH)

    def s_copy(source, target):
        return pltpu.make_async_remote_copy(
            src_ref=mine, dst_ref=sgath.at[source],
            send_sem=s_send.at[target], recv_sem=s_recv.at[source],
            device_id={"orient": target}, device_id_type=MESH)

    for t in range(1, n):
        d_copy(me, peer(t)).start()
    other_rows = [lax.rem(row + t, deep) for t in range(1, deep)]
    for c in order:
        if wide == 2:
            y_copy(c, row, col).start()
        for r in other_rows:
            z_copy(c, row, r).start()

    def relay(c):
        for r in other_rows:
            z_copy(c, r, r).wait_recv()
            if wide == 2:
                y_copy(c, r, col).start()

    def arrived(c):
        if wide == 2:
            y_copy(c, row, col).wait_recv()
            for r in other_rows:
                y_copy(c, r, col).wait_recv()

    eye8 = lax.broadcasted_iota(jnp.int32, (per, per), 0) == lax.broadcasted_iota(jnp.int32, (per, per), 1)
    group = max(1, ROWS // per)

    def ctf_piece(k):
        index = k * size + lax.broadcasted_iota(jnp.int32, (1, size), 1)
        row_pos = lax.shift_right_logical(index, 7).astype(jnp.float32)
        col_pos = ((index & 127) - 64).astype(jnp.float32)
        freq = math.pi * (row_pos * row_pos + col_pos * col_pos) / 16384.0
        noise_row = noise[:, cut(k)]

        def body(i):
            columns = []
            for j in range(group):
                line = dgath[i * group + j]
                columns.append(jnp.sum(jnp.where(eye8, line, 0.0), axis=1, keepdims=True))
            d = jnp.concatenate(columns, axis=0)
            value = -sin_of(d * freq + 0.07)
            rows = pl.ds(pl.multiple_of(i * ROWS, ROWS), ROWS)
            ctf[rows, cut(k)] = value
            ctf_power[rows, cut(k)] = (value * value * noise_row).astype(jnp.bfloat16)

        loop(parts // ROWS, body)

    def energy_piece(k):
        loads[k].wait()
        loads[k + PIECES].wait()

        def body(i):
            rows = pl.ds(pl.multiple_of(i * ROWS, ROWS), ROWS)
            re = refs[rows, cut(k)].astype(jnp.float32)
            im = refs[rows, cut(k + PIECES)].astype(jnp.float32)
            power[rows, :] = (re * re + im * im).astype(jnp.bfloat16)

        loop(ori // ROWS, body)
        term = -0.5 * lax.dot_general(ctf_power[:, cut(k)], power[...], DIMS, preferred_element_type=jnp.float32)
        if k == 0:
            acc[...] = term
        else:
            acc[...] += term

    def cross_piece(c):
        k = c % PIECES
        noise_row = noise[:, cut(k)]

        def body(i):
            rows = pl.ds(pl.multiple_of(i * ROWS, ROWS), ROWS)
            block = gath[pl.ds(i * group, group), :, cut(c)].astype(jnp.float32).reshape(ROWS, size)
            weighted[rows, :] = (block * ctf[rows, cut(k)] * noise_row).astype(jnp.bfloat16)

        loop(parts // ROWS, body)
        acc[...] += lax.dot_general(weighted[...], refs[:, cut(c)], DIMS, preferred_element_type=jnp.float32)

    for t in range(1, n):
        d_copy(peer(t), me).wait_recv()
    for k in range(PIECES):
        ctf_piece(k)
        relay(order[2 * k])
        energy_piece(k)
        relay(order[2 * k + 1])
    for c in order:
        arrived(c)
        cross_piece(c)

    scores = acc[...]
    top = jnp.max(scores, axis=1, keepdims=True)
    e = jnp.exp(scores - top)
    expon[:, :ori] = e
    eye = lax.broadcasted_iota(jnp.int32, (parts, parts), 0) == lax.broadcasted_iota(jnp.int32, (parts, parts), 1)

    def to_col(x):
        return jnp.sum(jnp.where(eye, x, 0), axis=1, keepdims=True)

    def to_row(x):
        return jnp.sum(jnp.where(eye, x, 0.0), axis=0, keepdims=True)

    start = to_col(starts[...])
    length = to_col(lens[...])
    ids = me * ori + lax.broadcasted_iota(jnp.int32, (parts, ori), 1)
    rel = ids - start
    inside = jnp.where(rel < 0, rel + total_ori, rel) < length
    first = me * ori - start
    first_inside = jnp.where(first < 0, first + total_ori, first) < length
    in_range = jnp.sum(jnp.where(inside, e, 0.0), axis=1, keepdims=True)
    ahead = jnp.sum(jnp.where(rel < 0, e, 0.0), axis=1, keepdims=True)
    ahead = jnp.where(first_inside, 0.0, ahead)
    for i, value in enumerate((top, jnp.sum(e, axis=1, keepdims=True), in_range, ahead)):
        line = to_row(value)
        mine[i : i + 1, :] = line
        sgath[me, i : i + 1, :] = line
    for t in range(1, n):
        s_copy(me, peer(t)).start()

    lanes = 128
    blocks = expon.shape[1] // lanes
    if ori < expon.shape[1]:
        expon[:, ori:] = jnp.zeros((parts, expon.shape[1] - ori), jnp.float32)
    upper = (
        lax.broadcasted_iota(jnp.int32, (lanes, lanes), 0) <= lax.broadcasted_iota(jnp.int32, (lanes, lanes), 1)
    ).astype(jnp.bfloat16)
    carry = jnp.zeros((parts, 1), jnp.float32)
    for b in range(blocks):
        x = expon[:, b * lanes : (b + 1) * lanes]
        high = x.astype(jnp.bfloat16)
        rest = x - high.astype(jnp.float32)
        mid = rest.astype(jnp.bfloat16)
        low = (rest - mid.astype(jnp.float32)).astype(jnp.bfloat16)
        run = carry
        for piece in (low, mid, high):
            run = run + jnp.dot(piece, upper, preferred_element_type=jnp.float32)
        prefix[:, b * lanes : (b + 1) * lanes] = run
        carry = run[:, lanes - 1 : lanes]

    for c in order:
        for r in other_rows:
            z_copy(c, row, r).wait_send()
            if wide == 2:
                y_copy(c, r, col).wait_send()
        if wide == 2:
            y_copy(c, row, col).wait_send()
    for t in range(1, n):
        d_copy(me, peer(t)).wait_send()
        s_copy(me, peer(t)).wait_send()
    for t in range(1, n):
        s_copy(peer(t), me).wait_recv()

    stats = [sgath[s] for s in range(n)]
    best = stats[0][0:1]
    for s in stats[1:]:
        best = jnp.maximum(best, s[0:1])
    scale = [jnp.exp(s[0:1] - best) for s in stats]
    base = jnp.zeros_like(best)
    my_base = base
    bases = []
    for s in range(n):
        my_base = jnp.where(me == s, base, my_base)
        bases.append(base)
        base = base + scale[s] * stats[s][1:2]
    total = base
    limit = thresholds[...].astype(jnp.float32) / 1024.0 * total
    kept = jnp.zeros_like(best)
    for s in range(n):
        left = limit - bases[s] - scale[s] * stats[s][3:4]
        kept = kept + jnp.minimum(jnp.maximum(left, 0.0), scale[s] * stats[s][2:3])
    kept_mass[...] = kept / total
    evidence[...] = best + jnp.log(total)
    my_scale = to_col(jnp.exp(mine[0:1, :] - best) / total)
    my_base = to_col(my_base / total)
    posterior[...] = expon[:, :ori] * my_scale
    cumulative[...] = my_base + prefix[:, :ori] * my_scale


def on_device(n, particles, defocus, inv_noise, references, thresholds, range_start, range_len):
    per, feat = particles.shape
    coef = feat // 2
    ori = references.shape[0]
    parts = n * per
    padded = -(-ori // 128) * 128
    chunks = 2 * PIECES
    deep = n // 2 if n % 2 == 0 else n
    f32, bf16 = jnp.float32, jnp.bfloat16
    vmem = pl.BlockSpec(memory_space=pltpu.VMEM)
    hbm = pl.BlockSpec(memory_space=pl.ANY)
    dma = pltpu.SemaphoreType.DMA
    outs = pl.pallas_call(
        functools.partial(kernel, n),
        out_shape=(
            jax.ShapeDtypeStruct((parts, ori), f32),
            jax.ShapeDtypeStruct((parts, ori), f32),
            jax.ShapeDtypeStruct((1, parts), f32),
            jax.ShapeDtypeStruct((1, parts), f32),
        ),
        in_specs=[hbm, hbm, vmem, hbm, vmem, vmem, vmem],
        out_specs=[vmem] * 4,
        scratch_shapes=[
            pltpu.VMEM((n, per, feat), bf16),
            pltpu.VMEM((n, 1, per), f32),
            pltpu.VMEM((ori, feat), bf16),
            pltpu.VMEM((parts, coef), f32),
            pltpu.VMEM((parts, coef), bf16),
            pltpu.VMEM((ori, coef // PIECES), bf16),
            pltpu.VMEM((parts, coef // PIECES), bf16),
            pltpu.VMEM((parts, ori), f32),
            pltpu.VMEM((parts, padded), f32),
            pltpu.VMEM((parts, padded), f32),
            pltpu.VMEM((4, parts), f32),
            pltpu.VMEM((n, 4, parts), f32),
            dma((2,)),
            dma((chunks,)),
            dma((chunks, deep)),
            dma((chunks, deep)),
            dma((chunks, deep)),
            dma((chunks, deep)),
            dma((n,)),
            dma((n,)),
            dma((n,)),
            dma((n,)),
        ],
        compiler_params=pltpu.CompilerParams(
            collective_id=0, has_side_effects=True, vmem_limit_bytes=56 * 1024 * 1024
        ),
    )(
        particles, defocus.reshape(1, per), inv_noise.reshape(1, coef), references,
        thresholds.reshape(1, parts), range_start.reshape(1, parts), range_len.reshape(1, parts),
    )
    return outs[0], outs[1], outs[2].reshape(parts), outs[3].reshape(parts)


def solution(mesh):
    return jax.shard_map(
        functools.partial(on_device, mesh.shape["orient"]),
        mesh=mesh,
        in_specs=(
            P(("dom", "orient"), None),
            P(("dom", "orient")),
            P(),
            P(("dom", "orient"), None),
            P("dom"),
            P("dom"),
            P("dom"),
        ),
        out_specs=(P("dom", "orient"), P("dom", "orient"), P("dom"), P("dom")),
        check_vma=False,
    )
```

```python
import functools
import math

import jax
import jax.numpy as jnp
from jax import lax
from jax.experimental import pallas as pl
from jax.experimental.pallas import tpu as pltpu
from jax.sharding import PartitionSpec as P

MESH = pl.DeviceIdType.MESH
DIMS = (((1,), (1,)), ((), ()))
PIECES = 3
ROWS = 16


def sin_of(x):
    k = jnp.floor(x * (1.0 / math.pi) + 0.5)
    r = x - k * 3.140625
    r = r - k * 9.67502593994140625e-4
    r = r - k * 1.509957990978376432e-7
    s = r * r
    p = jnp.float32(-2.3889859e-8)
    p = p * s + 2.7525562e-6
    p = p * s - 1.9840874e-4
    p = p * s + 8.3333310e-3
    p = p * s - 1.6666667e-1
    y = r + r * s * p
    half = k * 0.5
    return jnp.where(half == jnp.floor(half), y, -y)


def loop(count, body):
    if count <= 4:
        for i in range(count):
            body(i)
    else:
        def step(i, carry):
            body(i)
            return carry
        lax.fori_loop(0, count, step, 0)


def kernel(
    n, particles, defocus, noise_hbm, references, starts_hbm, lens_hbm,
    expon_hbm, prefix_hbm, sgath,
    gath, dgath, refs, ctf, ctf_power, power, weighted, acc, mine, expon, prefix, noise, starts, lens,
    own_sem, ref_sem, up_send, down_send, side_send, recv, dup_send, ddown_send, dside_send, d_recv, s_send, s_recv,
):
    wide = 2
    deep = n // wide
    per = particles.shape[0]
    feat = particles.shape[1]
    coef = feat // 2
    size = coef // PIECES
    ori = references.shape[0]
    total_ori = n * ori
    parts = n * per
    group = wide * per
    me = lax.axis_index("orient")
    row = lax.div(me, wide)
    col = lax.rem(me, wide)
    partner = row * wide + (1 - col)
    has_up = row + 1 < deep
    has_down = row > 0

    def cut(c):
        return pl.ds(c * size, size)

    def peer(t):
        return lax.rem(me + t, n)

    def near(act):
        act(partner)

        @pl.when(has_up)
        def _():
            act(me + wide)

        @pl.when(has_down)
        def _():
            act(me - wide)

    barrier = pltpu.get_barrier_semaphore()

    def greet(target):
        pl.semaphore_signal(barrier, inc=1, device_id={"orient": target}, device_id_type=MESH)

    near(greet)
    order = [c for k in range(PIECES) for c in (k, k + PIECES)]
    paired = order[-1]
    own = pltpu.make_async_copy(particles, gath.at[me], own_sem.at[0])
    own.start()
    own_d = pltpu.make_async_copy(defocus, dgath.at[me], own_sem.at[1])
    own_d.start()
    loads = {}
    for c in order:
        loads[c] = pltpu.make_async_copy(references.at[:, cut(c)], refs.at[:, cut(c)], ref_sem.at[c])
        loads[c].start()
    small = [
        pltpu.make_async_copy(noise_hbm, noise, own_sem.at[2]),
        pltpu.make_async_copy(starts_hbm, starts, own_sem.at[3]),
        pltpu.make_async_copy(lens_hbm, lens, own_sem.at[4]),
    ]
    for copy in small:
        copy.start()
    own.wait()
    own_d.wait()
    pl.semaphore_wait(barrier, 1 + has_up.astype(jnp.int32) + has_down.astype(jnp.int32))

    def remote(block, send_sem, recv_sem, target):
        return pltpu.make_async_remote_copy(
            src_ref=block, dst_ref=block, send_sem=send_sem, recv_sem=recv_sem,
            device_id={"orient": target}, device_id_type=MESH)

    def up(c, source):
        if c is None:
            return remote(dgath.at[source], dup_send.at[source], d_recv.at[source], me + wide)
        return remote(gath.at[source, :, cut(c)], up_send.at[c, source], recv.at[c, source], me + wide)

    def down(c, source):
        if c is None:
            return remote(dgath.at[source], ddown_send.at[source], d_recv.at[source], me - wide)
        return remote(gath.at[source, :, cut(c)], down_send.at[c, source], recv.at[c, source], me - wide)

    def side(c, source):
        if c is None:
            return remote(dgath.at[source], dside_send.at[source], d_recv.at[source], partner)
        return remote(gath.at[source, :, cut(c)], side_send.at[c, source], recv.at[c, source], partner)

    def s_copy(source, target):
        return pltpu.make_async_remote_copy(
            src_ref=mine, dst_ref=sgath.at[source],
            send_sem=s_send.at[target], recv_sem=s_recv.at[source],
            device_id={"orient": target}, device_id_type=MESH)

    def both(c, source):
        @pl.when(has_up)
        def _():
            up(c, source).start()

        @pl.when(has_down)
        def _():
            down(c, source).start()

    side(None, me).start()
    both(None, me)
    for c in [paired] + order[:-1]:
        side(c, me).start()
    for c in order:
        both(c, me)

    def handle(c, t):
        @pl.when(row >= t)
        def _():
            for column in (col, 1 - col) if c == paired else (col,):
                source = (row - t) * wide + column
                side(c, source).wait_recv()

                @pl.when(has_up)
                def _():
                    up(c, source).start()

                if c != paired:
                    side(c, source).start()

        @pl.when(row + t < deep)
        def _():
            for column in (col, 1 - col) if c == paired else (col,):
                source = (row + t) * wide + column
                side(c, source).wait_recv()

                @pl.when(has_down)
                def _():
                    down(c, source).start()

                if c != paired:
                    side(c, source).start()

    def arrived(c):
        if c != paired:
            for r in range(deep):
                side(c, r * wide + 1 - col).wait_recv()

    eye8 = lax.broadcasted_iota(jnp.int32, (per, per), 0) == lax.broadcasted_iota(jnp.int32, (per, per), 1)

    def ctf_row(r, wait=True):
        if wait:
            side(None, r * wide + 1 - col).wait_recv()
        columns = []
        for j in range(wide):
            columns.append(jnp.sum(jnp.where(eye8, dgath[r * wide + j], 0.0), axis=1, keepdims=True))
        d = jnp.concatenate(columns, axis=0)
        rows = pl.ds(pl.multiple_of(r * group, group), group)

        def body(k):
            index = k * size + lax.broadcasted_iota(jnp.int32, (1, size), 1)
            row_pos = lax.shift_right_logical(index, 7).astype(jnp.float32)
            col_pos = ((index & 127) - 64).astype(jnp.float32)
            freq = math.pi * (row_pos * row_pos + col_pos * col_pos) / 16384.0
            value = -sin_of(d * freq + 0.07)
            ctf[rows, cut(k)] = value
            ctf_power[rows, cut(k)] = (value * value * noise[cut(k)].reshape(1, size)).astype(jnp.bfloat16)

        for k in range(PIECES):
            body(k)

    def ctf_rows(t):
        @pl.when(row >= t)
        def _():
            ctf_row(row - t)

        @pl.when(row + t < deep)
        def _():
            ctf_row(row + t)

    def power_piece(k):
        loads[k].wait()
        loads[k + PIECES].wait()

        def body(i):
            rows = pl.ds(pl.multiple_of(i * ROWS, ROWS), ROWS)
            re = refs[rows, cut(k)].astype(jnp.float32)
            im = refs[rows, cut(k + PIECES)].astype(jnp.float32)
            power[rows, cut(k)] = (re * re + im * im).astype(jnp.bfloat16)

        loop(ori // ROWS, body)

    def energy_piece(k):
        term = -0.5 * lax.dot_general(
            ctf_power[:, cut(k)], power[:, cut(k)], DIMS, preferred_element_type=jnp.float32)
        if k == 0:
            acc[...] = term
        else:
            acc[...] += term

    def cross_piece(c):
        k = c % PIECES

        def body(i):
            rows = pl.ds(pl.multiple_of(i * group, group), group)
            block = gath[pl.ds(i * wide, wide), :, cut(c)].astype(jnp.float32).reshape(group, size)
            weighted[rows, :] = (block * ctf[rows, cut(k)] * noise[cut(k)].reshape(1, size)).astype(jnp.bfloat16)

        loop(deep, body)
        acc[...] += lax.dot_general(weighted[...], refs[:, cut(c)], DIMS, preferred_element_type=jnp.float32)

    short = deep == 4
    power_piece(0)
    power_piece(1)
    for copy in small:
        copy.wait()
    side(paired, partner).wait_recv()
    both(paired, partner)
    if short:
        tasks = {
            (1, 0): [lambda: ctf_row(row)], (1, 3): [lambda: power_piece(2)],
            (1, 5): [lambda: ctf_rows(1)], (2, 3): [lambda: ctf_rows(2)],
        }
        last = [lambda: ctf_rows(3)]
        last += [functools.partial(energy_piece, k) for k in range(PIECES)]
        for i, task in enumerate(last):
            tasks.setdefault((deep - 1, min(1 + i, len(order) - 1)), []).append(task)
    else:
        tasks = {(1, 0): [lambda: power_piece(2)]}
    for t in range(1, deep):
        handle(None, t)
        for i, c in enumerate(order):
            handle(c, t)
            for task in tasks.get((t, i), ()):
                task()
    if not short:
        for r in range(deep):
            side(None, r * wide + 1 - col).wait_recv()
        loop(deep, lambda r: ctf_row(r, wait=False))
        for k in range(PIECES):
            energy_piece(k)
    for c in order:
        arrived(c)
        cross_piece(c)

    scores = acc[...]
    top = jnp.max(scores, axis=1, keepdims=True)
    e = jnp.exp(scores - top)
    expon[:, :ori] = e
    eye = lax.broadcasted_iota(jnp.int32, (parts, parts), 0) == lax.broadcasted_iota(jnp.int32, (parts, parts), 1)

    def to_col(x):
        return jnp.sum(jnp.where(eye, x, 0), axis=1, keepdims=True)

    def to_row(x):
        return jnp.sum(jnp.where(eye, x, 0.0), axis=0, keepdims=True)

    start = to_col(starts[...])
    length = to_col(lens[...])
    ids = me * ori + lax.broadcasted_iota(jnp.int32, (parts, ori), 1)
    rel = ids - start
    inside = jnp.where(rel < 0, rel + total_ori, rel) < length
    first = me * ori - start
    first_inside = jnp.where(first < 0, first + total_ori, first) < length
    in_range = jnp.sum(jnp.where(inside, e, 0.0), axis=1, keepdims=True)
    ahead = jnp.sum(jnp.where(rel < 0, e, 0.0), axis=1, keepdims=True)
    ahead = jnp.where(first_inside, 0.0, ahead)
    for i, value in enumerate((top, jnp.sum(e, axis=1, keepdims=True), in_range, ahead)):
        line = to_row(value)
        mine[i : i + 1, :] = line
        sgath[me, i : i + 1, :] = line
    for t in range(1, n):
        s_copy(me, peer(t)).start()

    lanes = 128
    blocks = expon.shape[1] // lanes
    if ori < expon.shape[1]:
        expon[:, ori:] = jnp.zeros((parts, expon.shape[1] - ori), jnp.float32)
    upper = (
        lax.broadcasted_iota(jnp.int32, (lanes, lanes), 0) <= lax.broadcasted_iota(jnp.int32, (lanes, lanes), 1)
    ).astype(jnp.bfloat16)
    carry = jnp.zeros((parts, 1), jnp.float32)
    for b in range(blocks):
        x = expon[:, b * lanes : (b + 1) * lanes]
        high = x.astype(jnp.bfloat16)
        rest = x - high.astype(jnp.float32)
        mid = rest.astype(jnp.bfloat16)
        low = (rest - mid.astype(jnp.float32)).astype(jnp.bfloat16)
        run = carry
        for piece in (low, mid, high):
            run = run + jnp.dot(piece, upper, preferred_element_type=jnp.float32)
        prefix[:, b * lanes : (b + 1) * lanes] = run
        carry = run[:, lanes - 1 : lanes]

    outs = [
        pltpu.make_async_copy(expon, expon_hbm, own_sem.at[0]),
        pltpu.make_async_copy(prefix, prefix_hbm, own_sem.at[1]),
    ]
    for copy in outs:
        copy.start()

    def drain(c, source, along, across):
        if along:
            @pl.when(has_up & (lax.div(source, wide) <= row))
            def _():
                up(c, source).wait_send()

            @pl.when(has_down & (lax.div(source, wide) >= row))
            def _():
                down(c, source).wait_send()

        if across:
            side(c, source).wait_send()

    for c in [None] + order:
        for r in range(deep):
            drain(c, r * wide + col, True, c != paired)
            if c == paired:
                drain(c, r * wide + 1 - col, True, False)
    side(paired, me).wait_send()
    for t in range(1, n):
        s_copy(me, peer(t)).wait_send()
    for copy in outs:
        copy.wait()
    for t in range(1, n):
        s_copy(peer(t), me).wait_recv()


def finish(n, expon, prefix, sgath, thresholds, posterior, cumulative, evidence, kept_mass):
    parts, ori = posterior.shape
    me = lax.axis_index("orient")
    eye = lax.broadcasted_iota(jnp.int32, (parts, parts), 0) == lax.broadcasted_iota(jnp.int32, (parts, parts), 1)

    def to_col(x):
        return jnp.sum(jnp.where(eye, x, 0), axis=1, keepdims=True)

    stats = [sgath[s] for s in range(n)]
    best = stats[0][0:1]
    for s in stats[1:]:
        best = jnp.maximum(best, s[0:1])
    scale = [jnp.exp(s[0:1] - best) for s in stats]
    base = jnp.zeros_like(best)
    my_base = base
    bases = []
    for s in range(n):
        my_base = jnp.where(me == s, base, my_base)
        bases.append(base)
        base = base + scale[s] * stats[s][1:2]
    total = base
    limit = thresholds[...].astype(jnp.float32) / 1024.0 * total
    kept = jnp.zeros_like(best)
    for s in range(n):
        left = limit - bases[s] - scale[s] * stats[s][3:4]
        kept = kept + jnp.minimum(jnp.maximum(left, 0.0), scale[s] * stats[s][2:3])
    kept_mass[...] = kept / total
    evidence[...] = best + jnp.log(total)
    my_scale = to_col(jnp.exp(sgath[me, 0:1, :] - best) / total)
    my_base = to_col(my_base / total)
    posterior[...] = expon[:, :ori] * my_scale
    cumulative[...] = my_base + prefix[:, :ori] * my_scale


def on_device(n, particles, defocus, inv_noise, references, thresholds, range_start, range_len):
    per, feat = particles.shape
    coef = feat // 2
    ori = references.shape[0]
    parts = n * per
    padded = -(-ori // 128) * 128
    chunks = 2 * PIECES
    f32, bf16 = jnp.float32, jnp.bfloat16
    vmem = pl.BlockSpec(memory_space=pltpu.VMEM)
    hbm = pl.BlockSpec(memory_space=pl.ANY)
    dma = pltpu.SemaphoreType.DMA
    expon, prefix, stats = pl.pallas_call(
        functools.partial(kernel, n),
        out_shape=(
            jax.ShapeDtypeStruct((parts, padded), f32),
            jax.ShapeDtypeStruct((parts, padded), f32),
            jax.ShapeDtypeStruct((n, 4, parts), f32),
        ),
        in_specs=[hbm] * 6,
        out_specs=[hbm, hbm, vmem],
        scratch_shapes=[
            pltpu.VMEM((n, per, feat), bf16),
            pltpu.VMEM((n, 1, per), f32),
            pltpu.VMEM((ori, feat), bf16),
            pltpu.VMEM((parts, coef), f32),
            pltpu.VMEM((parts, coef), bf16),
            pltpu.VMEM((ori, coef), bf16),
            pltpu.VMEM((parts, coef // PIECES), bf16),
            pltpu.VMEM((parts, ori), f32),
            pltpu.VMEM((4, parts), f32),
            pltpu.VMEM((parts, padded), f32),
            pltpu.VMEM((parts, padded), f32),
            pltpu.VMEM((coef,), f32),
            pltpu.VMEM((1, parts), jnp.int32),
            pltpu.VMEM((1, parts), jnp.int32),
            dma((5,)),
            dma((chunks,)),
            dma((chunks, n)),
            dma((chunks, n)),
            dma((chunks, n)),
            dma((chunks, n)),
            dma((n,)),
            dma((n,)),
            dma((n,)),
            dma((n,)),
            dma((n,)),
            dma((n,)),
        ],
        compiler_params=pltpu.CompilerParams(
            collective_id=0, has_side_effects=True, vmem_limit_bytes=56 * 1024 * 1024
        ),
    )(
        particles, defocus.reshape(1, per), inv_noise, references,
        range_start.reshape(1, parts), range_len.reshape(1, parts),
    )
    outs = pl.pallas_call(
        functools.partial(finish, n),
        out_shape=(
            jax.ShapeDtypeStruct((parts, ori), f32),
            jax.ShapeDtypeStruct((parts, ori), f32),
            jax.ShapeDtypeStruct((1, parts), f32),
            jax.ShapeDtypeStruct((1, parts), f32),
        ),
        in_specs=[vmem] * 4,
        out_specs=[vmem] * 4,
    )(expon, prefix, stats, thresholds.reshape(1, parts))
    return outs[0], outs[1], outs[2].reshape(parts), outs[3].reshape(parts)


def solution(mesh):
    return jax.shard_map(
        functools.partial(on_device, mesh.shape["orient"]),
        mesh=mesh,
        in_specs=(
            P(("dom", "orient"), None),
            P(("dom", "orient")),
            P(),
            P(("dom", "orient"), None),
            P("dom"),
            P("dom"),
            P("dom"),
        ),
        out_specs=(P("dom", "orient"), P("dom", "orient"), P("dom"), P("dom")),
        check_vma=False,
    )
```

```python
import functools
import math

import jax
import jax.numpy as jnp
from jax import lax
from jax.experimental import pallas as pl
from jax.experimental.pallas import tpu as pltpu
from jax.sharding import PartitionSpec as P

MESH = pl.DeviceIdType.MESH
DIMS = (((1,), (1,)), ((), ()))
PIECES = 3
SPANS = ((0, 4), (4, 6))
ROWS = 16


def sin_of(x):
    k = jnp.floor(x * (1.0 / math.pi) + 0.5)
    r = x - k * 3.140625
    r = r - k * 9.67502593994140625e-4
    r = r - k * 1.509957990978376432e-7
    s = r * r
    p = jnp.float32(-2.3889859e-8)
    p = p * s + 2.7525562e-6
    p = p * s - 1.9840874e-4
    p = p * s + 8.3333310e-3
    p = p * s - 1.6666667e-1
    y = r + r * s * p
    half = k * 0.5
    return jnp.where(half == jnp.floor(half), y, -y)


def loop(count, body):
    if count <= 4:
        for i in range(count):
            body(i)
    else:
        def step(i, carry):
            body(i)
            return carry
        lax.fori_loop(0, count, step, 0)


def kernel(
    n, particles, defocus, noise_hbm, references, starts_hbm, lens_hbm,
    expon_hbm, prefix_hbm, sgath,
    gath, dgath, refs, ctf, ctf_power, power, weighted, acc, mine, expon, prefix, noise, starts, lens,
    own_sem, ref_sem, up_send, down_send, side_send, recv, dup_send, ddown_send, dside_send, d_recv, s_send, s_recv,
):
    wide = 2
    deep = n // wide
    per = particles.shape[0]
    feat = particles.shape[1]
    coef = feat // 2
    size = coef // PIECES
    ori = references.shape[0]
    total_ori = n * ori
    parts = n * per
    group = wide * per
    me = lax.axis_index("orient")
    row = lax.div(me, wide)
    col = lax.rem(me, wide)
    partner = row * wide + (1 - col)
    has_up = row + 1 < deep
    has_down = row > 0

    def cut(c):
        return pl.ds(c * size, size)

    def span(c):
        return pl.ds(SPANS[c][0] * size, (SPANS[c][1] - SPANS[c][0]) * size)

    def peer(t):
        return lax.rem(me + t, n)

    def near(act):
        act(partner)

        @pl.when(has_up)
        def _():
            act(me + wide)

        @pl.when(has_down)
        def _():
            act(me - wide)

    barrier = pltpu.get_barrier_semaphore()

    def greet(target):
        pl.semaphore_signal(barrier, inc=1, device_id={"orient": target}, device_id_type=MESH)

    near(greet)
    order = list(range(len(SPANS)))
    paired = -1
    pieces = [c for k in range(PIECES) for c in (k, k + PIECES)]
    own = pltpu.make_async_copy(particles, gath.at[me], own_sem.at[0])
    own.start()
    own_d = pltpu.make_async_copy(defocus, dgath.at[me], own_sem.at[1])
    own_d.start()
    loads = {}
    for c in pieces:
        loads[c] = pltpu.make_async_copy(references.at[:, cut(c)], refs.at[:, cut(c)], ref_sem.at[c])
        loads[c].start()
    small = [
        pltpu.make_async_copy(noise_hbm, noise, own_sem.at[2]),
        pltpu.make_async_copy(starts_hbm, starts, own_sem.at[3]),
        pltpu.make_async_copy(lens_hbm, lens, own_sem.at[4]),
    ]
    for copy in small:
        copy.start()
    own.wait()
    own_d.wait()
    pl.semaphore_wait(barrier, 1 + has_up.astype(jnp.int32) + has_down.astype(jnp.int32))

    def remote(block, send_sem, recv_sem, target):
        return pltpu.make_async_remote_copy(
            src_ref=block, dst_ref=block, send_sem=send_sem, recv_sem=recv_sem,
            device_id={"orient": target}, device_id_type=MESH)

    def up(c, source):
        if c is None:
            return remote(dgath.at[source], dup_send.at[source], d_recv.at[source], me + wide)
        return remote(gath.at[source, :, span(c)], up_send.at[c, source], recv.at[c, source], me + wide)

    def down(c, source):
        if c is None:
            return remote(dgath.at[source], ddown_send.at[source], d_recv.at[source], me - wide)
        return remote(gath.at[source, :, span(c)], down_send.at[c, source], recv.at[c, source], me - wide)

    def side(c, source):
        if c is None:
            return remote(dgath.at[source], dside_send.at[source], d_recv.at[source], partner)
        return remote(gath.at[source, :, span(c)], side_send.at[c, source], recv.at[c, source], partner)

    def s_copy(source, target):
        return pltpu.make_async_remote_copy(
            src_ref=mine, dst_ref=sgath.at[source],
            send_sem=s_send.at[target], recv_sem=s_recv.at[source],
            device_id={"orient": target}, device_id_type=MESH)

    def both(c, source):
        @pl.when(has_up)
        def _():
            up(c, source).start()

        @pl.when(has_down)
        def _():
            down(c, source).start()

    side(None, me).start()
    both(None, me)
    for c in order:
        side(c, me).start()
    for c in order:
        both(c, me)

    def handle(c, t):
        @pl.when(row >= t)
        def _():
            for column in (col, 1 - col) if c == paired else (col,):
                source = (row - t) * wide + column
                side(c, source).wait_recv()

                @pl.when(has_up)
                def _():
                    up(c, source).start()

                if c != paired:
                    side(c, source).start()

        @pl.when(row + t < deep)
        def _():
            for column in (col, 1 - col) if c == paired else (col,):
                source = (row + t) * wide + column
                side(c, source).wait_recv()

                @pl.when(has_down)
                def _():
                    down(c, source).start()

                if c != paired:
                    side(c, source).start()

    def arrived(c):
        if c != paired:
            for r in range(deep):
                side(c, r * wide + 1 - col).wait_recv()

    eye8 = lax.broadcasted_iota(jnp.int32, (per, per), 0) == lax.broadcasted_iota(jnp.int32, (per, per), 1)

    def ctf_row(r, wait=True):
        if wait:
            side(None, r * wide + 1 - col).wait_recv()
        columns = []
        for j in range(wide):
            columns.append(jnp.sum(jnp.where(eye8, dgath[r * wide + j], 0.0), axis=1, keepdims=True))
        d = jnp.concatenate(columns, axis=0)
        rows = pl.ds(pl.multiple_of(r * group, group), group)

        def body(k):
            index = k * size + lax.broadcasted_iota(jnp.int32, (1, size), 1)
            row_pos = lax.shift_right_logical(index, 7).astype(jnp.float32)
            col_pos = ((index & 127) - 64).astype(jnp.float32)
            freq = math.pi * (row_pos * row_pos + col_pos * col_pos) / 16384.0
            value = -sin_of(d * freq + 0.07)
            ctf[rows, cut(k)] = value
            ctf_power[rows, cut(k)] = (value * value * noise[cut(k)].reshape(1, size)).astype(jnp.bfloat16)

        for k in range(PIECES):
            body(k)

    def ctf_rows(t):
        @pl.when(row >= t)
        def _():
            ctf_row(row - t)

        @pl.when(row + t < deep)
        def _():
            ctf_row(row + t)

    def power_piece(k):
        loads[k].wait()
        loads[k + PIECES].wait()

        def body(i):
            rows = pl.ds(pl.multiple_of(i * ROWS, ROWS), ROWS)
            re = refs[rows, cut(k)].astype(jnp.float32)
            im = refs[rows, cut(k + PIECES)].astype(jnp.float32)
            power[rows, cut(k)] = (re * re + im * im).astype(jnp.bfloat16)

        loop(ori // ROWS, body)

    def energy_piece(k):
        term = -0.5 * lax.dot_general(
            ctf_power[:, cut(k)], power[:, cut(k)], DIMS, preferred_element_type=jnp.float32)
        if k == 0:
            acc[...] = term
        else:
            acc[...] += term

    def cross_piece(c):
        k = c % PIECES

        def body(i):
            rows = pl.ds(pl.multiple_of(i * group, group), group)
            block = gath[pl.ds(i * wide, wide), :, cut(c)].astype(jnp.float32).reshape(group, size)
            weighted[rows, :] = (block * ctf[rows, cut(k)] * noise[cut(k)].reshape(1, size)).astype(jnp.bfloat16)

        loop(deep, body)
        acc[...] += lax.dot_general(weighted[...], refs[:, cut(c)], DIMS, preferred_element_type=jnp.float32)

    short = deep == 4
    power_piece(0)
    power_piece(1)
    for copy in small:
        copy.wait()
    if short:
        tasks = {
            (1, 0): [lambda: ctf_row(row)],
            (1, 1): [lambda: power_piece(2), lambda: ctf_rows(1)],
            (2, 1): [lambda: ctf_rows(2)],
            (3, 0): [lambda: ctf_rows(3), lambda: energy_piece(0)],
            (3, 1): [lambda: energy_piece(1), lambda: energy_piece(2)],
        }
    else:
        tasks = {(1, 0): [lambda: power_piece(2)]}
    for t in range(1, deep):
        handle(None, t)
        for i, c in enumerate(order):
            handle(c, t)
            for task in tasks.get((t, i), ()):
                task()
    if not short:
        for r in range(deep):
            side(None, r * wide + 1 - col).wait_recv()
        loop(deep, lambda r: ctf_row(r, wait=False))
        for k in range(PIECES):
            energy_piece(k)
    for c in order:
        arrived(c)
        for piece in range(*SPANS[c]):
            cross_piece(piece)

    scores = acc[...]
    top = jnp.max(scores, axis=1, keepdims=True)
    e = jnp.exp(scores - top)
    expon[:, :ori] = e
    eye = lax.broadcasted_iota(jnp.int32, (parts, parts), 0) == lax.broadcasted_iota(jnp.int32, (parts, parts), 1)

    def to_col(x):
        return jnp.sum(jnp.where(eye, x, 0), axis=1, keepdims=True)

    def to_row(x):
        return jnp.sum(jnp.where(eye, x, 0.0), axis=0, keepdims=True)

    start = to_col(starts[...])
    length = to_col(lens[...])
    ids = me * ori + lax.broadcasted_iota(jnp.int32, (parts, ori), 1)
    rel = ids - start
    inside = jnp.where(rel < 0, rel + total_ori, rel) < length
    first = me * ori - start
    first_inside = jnp.where(first < 0, first + total_ori, first) < length
    in_range = jnp.sum(jnp.where(inside, e, 0.0), axis=1, keepdims=True)
    ahead = jnp.sum(jnp.where(rel < 0, e, 0.0), axis=1, keepdims=True)
    ahead = jnp.where(first_inside, 0.0, ahead)
    for i, value in enumerate((top, jnp.sum(e, axis=1, keepdims=True), in_range, ahead)):
        line = to_row(value)
        mine[i : i + 1, :] = line
        sgath[me, i : i + 1, :] = line
    for t in range(1, n):
        s_copy(me, peer(t)).start()

    lanes = 128
    blocks = expon.shape[1] // lanes
    if ori < expon.shape[1]:
        expon[:, ori:] = jnp.zeros((parts, expon.shape[1] - ori), jnp.float32)
    upper = (
        lax.broadcasted_iota(jnp.int32, (lanes, lanes), 0) <= lax.broadcasted_iota(jnp.int32, (lanes, lanes), 1)
    ).astype(jnp.bfloat16)
    carry = jnp.zeros((parts, 1), jnp.float32)
    for b in range(blocks):
        x = expon[:, b * lanes : (b + 1) * lanes]
        high = x.astype(jnp.bfloat16)
        rest = x - high.astype(jnp.float32)
        mid = rest.astype(jnp.bfloat16)
        low = (rest - mid.astype(jnp.float32)).astype(jnp.bfloat16)
        run = carry
        for piece in (low, mid, high):
            run = run + jnp.dot(piece, upper, preferred_element_type=jnp.float32)
        prefix[:, b * lanes : (b + 1) * lanes] = run
        carry = run[:, lanes - 1 : lanes]

    outs = [
        pltpu.make_async_copy(expon, expon_hbm, own_sem.at[0]),
        pltpu.make_async_copy(prefix, prefix_hbm, own_sem.at[1]),
    ]
    for copy in outs:
        copy.start()

    def drain(c, source, along, across):
        if along:
            @pl.when(has_up & (lax.div(source, wide) <= row))
            def _():
                up(c, source).wait_send()

            @pl.when(has_down & (lax.div(source, wide) >= row))
            def _():
                down(c, source).wait_send()

        if across:
            side(c, source).wait_send()

    for c in [None] + order:
        for r in range(deep):
            drain(c, r * wide + col, True, c != paired)
            if c == paired:
                drain(c, r * wide + 1 - col, True, False)
    for t in range(1, n):
        s_copy(me, peer(t)).wait_send()
    for copy in outs:
        copy.wait()
    for t in range(1, n):
        s_copy(peer(t), me).wait_recv()


def finish(n, expon, prefix, sgath, thresholds, posterior, cumulative, evidence, kept_mass):
    parts, ori = posterior.shape
    me = lax.axis_index("orient")
    eye = lax.broadcasted_iota(jnp.int32, (parts, parts), 0) == lax.broadcasted_iota(jnp.int32, (parts, parts), 1)

    def to_col(x):
        return jnp.sum(jnp.where(eye, x, 0), axis=1, keepdims=True)

    stats = [sgath[s] for s in range(n)]
    best = stats[0][0:1]
    for s in stats[1:]:
        best = jnp.maximum(best, s[0:1])
    scale = [jnp.exp(s[0:1] - best) for s in stats]
    base = jnp.zeros_like(best)
    my_base = base
    bases = []
    for s in range(n):
        my_base = jnp.where(me == s, base, my_base)
        bases.append(base)
        base = base + scale[s] * stats[s][1:2]
    total = base
    limit = thresholds[...].astype(jnp.float32) / 1024.0 * total
    kept = jnp.zeros_like(best)
    for s in range(n):
        left = limit - bases[s] - scale[s] * stats[s][3:4]
        kept = kept + jnp.minimum(jnp.maximum(left, 0.0), scale[s] * stats[s][2:3])
    kept_mass[...] = kept / total
    evidence[...] = best + jnp.log(total)
    my_scale = to_col(jnp.exp(sgath[me, 0:1, :] - best) / total)
    my_base = to_col(my_base / total)
    posterior[...] = expon[:, :ori] * my_scale
    cumulative[...] = my_base + prefix[:, :ori] * my_scale


def on_device(n, particles, defocus, inv_noise, references, thresholds, range_start, range_len):
    per, feat = particles.shape
    coef = feat // 2
    ori = references.shape[0]
    parts = n * per
    padded = -(-ori // 128) * 128
    chunks = 2 * PIECES
    f32, bf16 = jnp.float32, jnp.bfloat16
    vmem = pl.BlockSpec(memory_space=pltpu.VMEM)
    hbm = pl.BlockSpec(memory_space=pl.ANY)
    dma = pltpu.SemaphoreType.DMA
    expon, prefix, stats = pl.pallas_call(
        functools.partial(kernel, n),
        out_shape=(
            jax.ShapeDtypeStruct((parts, padded), f32),
            jax.ShapeDtypeStruct((parts, padded), f32),
            jax.ShapeDtypeStruct((n, 4, parts), f32),
        ),
        in_specs=[hbm] * 6,
        out_specs=[hbm, hbm, vmem],
        scratch_shapes=[
            pltpu.VMEM((n, per, feat), bf16),
            pltpu.VMEM((n, 1, per), f32),
            pltpu.VMEM((ori, feat), bf16),
            pltpu.VMEM((parts, coef), f32),
            pltpu.VMEM((parts, coef), bf16),
            pltpu.VMEM((ori, coef), bf16),
            pltpu.VMEM((parts, coef // PIECES), bf16),
            pltpu.VMEM((parts, ori), f32),
            pltpu.VMEM((4, parts), f32),
            pltpu.VMEM((parts, padded), f32),
            pltpu.VMEM((parts, padded), f32),
            pltpu.VMEM((coef,), f32),
            pltpu.VMEM((1, parts), jnp.int32),
            pltpu.VMEM((1, parts), jnp.int32),
            dma((5,)),
            dma((chunks,)),
            dma((len(SPANS), n)),
            dma((len(SPANS), n)),
            dma((len(SPANS), n)),
            dma((len(SPANS), n)),
            dma((n,)),
            dma((n,)),
            dma((n,)),
            dma((n,)),
            dma((n,)),
            dma((n,)),
        ],
        compiler_params=pltpu.CompilerParams(
            collective_id=0, has_side_effects=True, vmem_limit_bytes=56 * 1024 * 1024
        ),
    )(
        particles, defocus.reshape(1, per), inv_noise, references,
        range_start.reshape(1, parts), range_len.reshape(1, parts),
    )
    outs = pl.pallas_call(
        functools.partial(finish, n),
        out_shape=(
            jax.ShapeDtypeStruct((parts, ori), f32),
            jax.ShapeDtypeStruct((parts, ori), f32),
            jax.ShapeDtypeStruct((1, parts), f32),
            jax.ShapeDtypeStruct((1, parts), f32),
        ),
        in_specs=[vmem] * 4,
        out_specs=[vmem] * 4,
    )(expon, prefix, stats, thresholds.reshape(1, parts))
    return outs[0], outs[1], outs[2].reshape(parts), outs[3].reshape(parts)


def solution(mesh):
    return jax.shard_map(
        functools.partial(on_device, mesh.shape["orient"]),
        mesh=mesh,
        in_specs=(
            P(("dom", "orient"), None),
            P(("dom", "orient")),
            P(),
            P(("dom", "orient"), None),
            P("dom"),
            P("dom"),
            P("dom"),
        ),
        out_specs=(P("dom", "orient"), P("dom", "orient"), P("dom"), P("dom")),
        check_vma=False,
    )
```
